32 devices in a mesh: lat: 2 (over core), lon: 2 (over y), lev: 2 (over x), unit: 4 (over z).
Axes of the slice: x: 2, y: 2, z: 4, core: 2. Of those that a mesh axis runs over, the one named last changes fastest.
Arguments:
- tracer: float32 [32, 256, 32, 128], P(('unit', 'lat'), 'lon', 'lev'), parts along dimension 0, may hold values from 0.5 to 2
- diffusivity: float32 [32, 256, 32, 128], P(('unit', 'lat'), 'lon', 'lev'), parts along dimension 0, may hold values from 0.03 to 0.15
- source: float32 [32, 256, 32, 128], P(('unit', 'lat'), 'lon', 'lev'), parts along dimension 0, may hold values from -0.2 to 0.2
Outputs:
- standardized: float32 [32, 256, 32, 128], P(('unit', 'lat'), 'lon', 'lev'), parts along dimension 0
- tracer_end: float32 [32, 256, 32, 128], P(('unit', 'lat'), 'lon', 'lev'), parts along dimension 0
The draws below stay inside these ranges and needn't reach their ends.
There are 4 independent parts, one for each index of `unit`. The reference program is written for one: setup_inputs(seed, part) draws one part's arguments, and reference() takes and returns one part's arrays. A program takes and returns all parts, laid end to end along the dimension named above; each array names one. Nothing has to cross between parts.
All inputs are finite; a program needn't handle non-finite values.
Results may differ from the reference program's by a relative error of at most 0.00002.
Values sent between devices are 32-bit elements; how exact they have to be, the bound alone decides.
A program may use at most 128 MiB of HBM per device.

```python
import jax
import jax.numpy as jnp
from jax import lax

GRID_J = 8
GRID_I = 256
GRID_K = 32
LEVELS = 128
STEPS = 4


def steps_of(rng, extent, split, smallest, largest):
    gain = 1.0
    for dim, parts in split:
        steps = jax.random.uniform(jax.random.fold_in(jax.random.fold_in(rng, 6), dim), (parts,), jnp.float32, smallest / len(split), largest / len(split))
        gain = gain * jnp.repeat(jnp.exp(steps), extent[dim] // parts).reshape((-1,) + (1,) * (len(extent) - 1 - dim))
    return gain


def setup_inputs(seed: int = 0, part: int = 0) -> dict:
    streams_of = jax.random.split(jax.random.key(seed), 4)
    part_keys = jax.random.split(jax.random.fold_in(streams_of[3], part), 4)
    return {
        "tracer": jnp.clip(0.5 + 1.5 * jax.random.uniform(part_keys[0], (GRID_J, GRID_I, GRID_K, LEVELS), jnp.float32) ** steps_of(part_keys[0], (GRID_J, GRID_I, GRID_K, LEVELS), ((0, 2), (1, 2), (2, 2)), -0.2, 0.2), 0.5, 2.0),
        "diffusivity": jnp.clip(0.03 + 0.120000007 * jax.random.uniform(part_keys[1], (GRID_J, GRID_I, GRID_K, LEVELS), jnp.float32) ** steps_of(part_keys[1], (GRID_J, GRID_I, GRID_K, LEVELS), ((0, 2), (1, 2), (2, 2)), -0.2, 0.2), 0.03, 0.15),
        "source": jnp.clip(jax.random.uniform(part_keys[2], (GRID_J, GRID_I, GRID_K, LEVELS), jnp.float32, -0.2, 0.2) * steps_of(part_keys[2], (GRID_J, GRID_I, GRID_K, LEVELS), ((0, 2), (1, 2), (2, 2)), -0.4, 0.0), -0.2, 0.2),
    }


def strip_edges(values, dims):
    for dim in dims:
        values = lax.slice_in_dim(values, 1, values.shape[dim] - 1, axis=dim)
    return values

def neighbour(values, dim, start, dims):
    others = [other for other in dims if other != dim]
    values = strip_edges(values, others)
    return lax.slice_in_dim(values, start, start + values.shape[dim] - 2, axis=dim)

def one_step(padded, diffusivity, source):
    middle = strip_edges(padded, (0, 1, 2))
    lower = [neighbour(padded, dim, 0, (0, 1, 2)) for dim in (0, 1, 2)]
    upper = [neighbour(padded, dim, 2, (0, 1, 2)) for dim in (0, 1, 2)]
    spread = lower[0] + upper[0] + lower[1] + upper[1] + lower[2] + upper[2] - 6.0 * middle
    return middle + diffusivity * spread + source

def reference(tracer, diffusivity, source):
    for step in range(STEPS):
        tracer = one_step(jnp.pad(tracer, ((1, 1), (1, 1), (1, 1), (0, 0)), mode='wrap'), diffusivity, source)
    line_mean = lax.optimization_barrier(jnp.mean(tracer, axis=2, keepdims=True))
    centred = tracer - line_mean
    line_variance = lax.optimization_barrier(jnp.mean(centred * centred, axis=2, keepdims=True))
    standardized = centred * lax.rsqrt(line_variance + 0.0001)
    return (standardized, tracer)
```

```python
import functools

import jax
import jax.numpy as jnp
from jax import lax
from jax.experimental import pallas as pl
from jax.experimental.pallas import tpu as pltpu
from jax.sharding import PartitionSpec as P

STEPS = 4
PAD = 8
EPSILON = 0.0001
MESH = pl.DeviceIdType.MESH


def rows_of(extent):
    for rows in (32, 16, 8):
        if extent % rows == 0:
            return rows
    return extent


def steps_kernel(
    sizes, shape, tracer, diffusivity, source, standardized, tracer_end,
    field, coeff, forcing, last, own, others,
    load_sem, lev_send, lev_recv, lat_send, lat_recv, lon_send, lon_recv, stat_send, stat_recv,
):
    n_j, n_i, n_k, _ = shape
    n_lat, n_lon, n_lev = sizes
    inner = pl.ds(PAD, n_i)
    whole_j = pl.ds(1, n_j)
    chunk = rows_of(n_i)
    lat, lon, lev = lax.axis_index("lat"), lax.axis_index("lon"), lax.axis_index("lev")
    lat_up, lat_down = lax.rem(lat + 1, n_lat), lax.rem(lat + n_lat - 1, n_lat)
    lon_up, lon_down = lax.rem(lon + 1, n_lon), lax.rem(lon + n_lon - 1, n_lon)
    lev_up, lev_down = lax.rem(lev + 1, n_lev), lax.rem(lev + n_lev - 1, n_lev)

    def load(which, k):
        array = (tracer, diffusivity, source)[which]
        if which == 0:
            target = field.at[0, k + 1, whole_j, inner, :]
        else:
            target = (coeff, forcing)[which - 1].at[k]
        return pltpu.make_async_copy(array.at[:, :, k, :], target, load_sem.at[which, k])

    def remote(src, dst, send, recv, device):
        return pltpu.make_async_remote_copy(
            src_ref=src, dst_ref=dst, send_sem=send, recv_sem=recv,
            device_id=device, device_id_type=MESH,
        )

    def lev_copies(step, j):
        down = remote(
            field.at[step, 1, j, inner, :], field.at[step, n_k + 1, j, inner, :],
            lev_send.at[step, j - 1, 0], lev_recv.at[step, j - 1, 0], {"lev": lev_down},
        )
        up = remote(
            field.at[step, n_k, j, inner, :], field.at[step, 0, j, inner, :],
            lev_send.at[step, j - 1, 1], lev_recv.at[step, j - 1, 1], {"lev": lev_up},
        )
        return down, up

    parts = (pl.ds(1, 1), pl.ds(n_k, 1), pl.ds(2, n_k - 2))

    def lat_copy(step, part, side):
        k = parts[part]
        src, dst, to = ((1, n_j + 1, lat_down), (n_j, 0, lat_up))[side]
        return remote(
            field.at[step, k, src, inner, :], field.at[step, k, dst, inner, :],
            lat_send.at[step, part, side], lat_recv.at[step, part, side], {"lat": to},
        )

    def lon_copy(step, part, side):
        k = parts[part]
        src, dst, to = (
            (PAD, PAD + n_i, lon_down), (PAD + n_i - 1, PAD - 1, lon_up)
        )[side]
        return remote(
            field.at[step, k, whole_j, pl.ds(src, 1), :],
            field.at[step, k, whole_j, pl.ds(dst, 1), :],
            lon_send.at[step, part, side], lon_recv.at[step, part, side], {"lon": to},
        )

    def stat_copies(j):
        return [
            remote(
                own.at[j - 1], others.at[n_lev - 1 - away, j - 1],
                stat_send.at[away - 1, j - 1], stat_recv.at[n_lev - 1 - away, j - 1],
                {"lev": lax.rem(lev + away, n_lev)},
            )
            for away in range(1, n_lev)
        ]

    def update(step, k, j):
        for low in range(0, n_i, chunk):
            r = PAD + low
            middle = field[step, k, j, pl.ds(r, chunk), :]
            spread = (
                field[step, k, j - 1, pl.ds(r, chunk), :] + field[step, k, j + 1, pl.ds(r, chunk), :]
                + field[step, k, j, pl.ds(r - 1, chunk), :] + field[step, k, j, pl.ds(r + 1, chunk), :]
                + field[step, k - 1, j, pl.ds(r, chunk), :] + field[step, k + 1, j, pl.ds(r, chunk), :]
                - 6.0 * middle
            )
            rows = pl.ds(low, chunk)
            value = middle + coeff[k - 1, j - 1, rows, :] * spread + forcing[k - 1, j - 1, rows, :]
            if step == STEPS - 1:
                last[k - 1, j - 1, rows, :] = value
                place = pl.ds(low * n_k + k - 1, chunk, stride=n_k)
                tracer_end[j - 1, place, :] = value
            else:
                field[step + 1, k, j, pl.ds(r, chunk), :] = value

    def summarise(j):
        for low in range(0, n_i, chunk):
            rows = pl.ds(low, chunk)
            total = last[0, j - 1, rows, :]
            for k in range(1, n_k):
                total = total + last[k, j - 1, rows, :]
            mean = total * (1.0 / n_k)
            squares = jnp.zeros_like(mean)
            for k in range(n_k):
                moved = last[k, j - 1, rows, :] - mean
                squares = squares + moved * moved
            own[j - 1, 0, rows, :] = mean
            own[j - 1, 1, rows, :] = squares

    def combine(j):
        for low in range(0, n_i, chunk):
            rows = pl.ds(low, chunk)
            means = [own[j - 1, 0, rows, :]] + [others[p, j - 1, 0, rows, :] for p in range(n_lev - 1)]
            mean = functools.reduce(jnp.add, means) * (1.0 / n_lev)
            squares = own[j - 1, 1, rows, :]
            for p in range(n_lev - 1):
                squares = squares + others[p, j - 1, 1, rows, :]
            for part in means:
                squares = squares + n_k * ((part - mean) * (part - mean))
            scale = lax.rsqrt(squares * (1.0 / (n_k * n_lev)) + EPSILON)
            for k in range(n_k):
                place = pl.ds(low * n_k + k, chunk, stride=n_k)
                standardized[j - 1, place, :] = (last[k, j - 1, rows, :] - mean) * scale

    def over_k(first, end, body):
        def wrapped(k, carry):
            body(k)
            return carry
        lax.fori_loop(first, end, wrapped, 0)

    edges = (0, n_k - 1)
    for k in edges:
        load(0, k).start()

    barrier = pltpu.get_barrier_semaphore()
    greeted = (
        [{"lat": lax.rem(lat + a, n_lat)} for a in sorted({1, n_lat - 1})]
        + [{"lon": lax.rem(lon + a, n_lon)} for a in sorted({1, n_lon - 1})]
        + [{"lev": lax.rem(lev + a, n_lev)} for a in range(1, n_lev)]
    )
    for device in greeted:
        pl.semaphore_signal(barrier, inc=1, device_id=device, device_id_type=MESH)
    pl.semaphore_wait(barrier, len(greeted))

    for k in edges:
        load(0, k).wait()
    for j in range(1, n_j + 1):
        for copy in lev_copies(0, j):
            copy.start()
    for k in (1, n_k - 2):
        load(0, k).start()
    for which in (1, 2):
        for k in edges:
            load(which, k).start()
    over_k(2, n_k - 2, lambda k: load(0, k).start())
    for which in (1, 2):
        over_k(1, n_k - 1, lambda k: load(which, k).start())
    for part in (0, 1):
        for side in (0, 1):
            lat_copy(0, part, side).start()
            lon_copy(0, part, side).start()
    for k in (1, n_k - 2):
        load(0, k).wait()
    for which in (1, 2):
        for k in edges:
            load(which, k).wait()

    def inside(step):
        for side in (0, 1):
            lat_copy(step, 2, side).wait_recv()
            lon_copy(step, 2, side).wait_recv()

        def body(k):
            if step == 0:
                for which in (1, 2):
                    load(which, k - 1).wait()

            def across(j, carry):
                update(step, k, j)
                return carry
            lax.fori_loop(1, n_j + 1, across, 0)

        over_k(2, n_k, body)
        if step < STEPS - 1:
            for side in (0, 1):
                lat_copy(step + 1, 2, side).start()
                lon_copy(step + 1, 2, side).start()

    def outside(step):
        for part in (0, 1):
            for side in (0, 1):
                lat_copy(step, part, side).wait_recv()
                lon_copy(step, part, side).wait_recv()
        for j in range(1, n_j + 1):
            for copy in lev_copies(step, j):
                copy.wait_recv()
            update(step, 1, j)
            update(step, n_k, j)
            if step < STEPS - 1:
                for copy in lev_copies(step + 1, j):
                    copy.start()
                for side, edge in ((0, 1), (1, n_j)):
                    if j == edge:
                        for part in (0, 1):
                            lat_copy(step + 1, part, side).start()
            else:
                summarise(j)
                for copy in stat_copies(j):
                    copy.start()
        if step < STEPS - 1:
            for part in (0, 1):
                for side in (0, 1):
                    lon_copy(step + 1, part, side).start()

    over_k(2, n_k - 2, lambda k: load(0, k).wait())
    for side in (0, 1):
        lat_copy(0, 2, side).start()
        lon_copy(0, 2, side).start()
    for step in range(STEPS):
        inside(step)
        outside(step)
    for j in range(1, n_j + 1):
        for copy in stat_copies(j):
            copy.wait_recv()
        combine(j)

    for step in range(STEPS):
        for j in range(1, n_j + 1):
            for copy in lev_copies(step, j):
                copy.wait_send()
        for part in range(3):
            for side in (0, 1):
                lat_copy(step, part, side).wait_send()
                lon_copy(step, part, side).wait_send()
    for j in range(1, n_j + 1):
        for copy in stat_copies(j):
            copy.wait_send()


def write_kernel(first, second, first_out, second_out, sem):
    copies = [
        pltpu.make_async_copy(src.at[j], dst.at[j], sem.at[which, j])
        for j in range(first.shape[0])
        for which, (src, dst) in enumerate(((first, first_out), (second, second_out)))
    ]
    for copy in copies:
        copy.start()
    for copy in copies:
        copy.wait()


def on_device(sizes, tracer, diffusivity, source):
    shape = tracer.shape
    n_j, n_i, n_k, levels = shape
    n_lev = sizes[2]
    f32 = jnp.float32
    sem = pltpu.SemaphoreType.DMA
    standardized, tracer_end = pl.pallas_call(
        functools.partial(steps_kernel, sizes, shape),
        out_shape=(
            pltpu.VMEM((n_j, n_i * n_k, levels), f32),
            pltpu.VMEM((n_j, n_i * n_k, levels), f32),
        ),
        in_specs=[pl.BlockSpec(memory_space=pl.ANY)] * 3,
        out_specs=(pl.BlockSpec(memory_space=pltpu.VMEM),) * 2,
        scratch_shapes=[
            pltpu.VMEM((STEPS, n_k + 2, n_j + 2, n_i + 2 * PAD, levels), f32),
            pltpu.VMEM((n_k, n_j, n_i, levels), f32),
            pltpu.VMEM((n_k, n_j, n_i, levels), f32),
            pltpu.VMEM((n_k, n_j, n_i, levels), f32),
            pltpu.VMEM((n_j, 2, n_i, levels), f32),
            pltpu.VMEM((n_lev - 1, n_j, 2, n_i, levels), f32),
            sem((3, n_k)),
            sem((STEPS, n_j, 2)), sem((STEPS, n_j, 2)),
            sem((STEPS, 3, 2)), sem((STEPS, 3, 2)),
            sem((STEPS, 3, 2)), sem((STEPS, 3, 2)),
            sem((n_lev - 1, n_j)), sem((n_lev - 1, n_j)),
        ],
        compiler_params=pltpu.CompilerParams(
            collective_id=0, has_side_effects=True, vmem_limit_bytes=48 * 1024 * 1024,
        ),
    )(tracer, diffusivity, source)
    flat = jax.ShapeDtypeStruct((n_j, n_i * n_k, levels), f32)
    standardized, tracer_end = pl.pallas_call(
        write_kernel,
        out_shape=(flat, flat),
        in_specs=[pl.BlockSpec(memory_space=pltpu.VMEM)] * 2,
        out_specs=(pl.BlockSpec(memory_space=pl.ANY),) * 2,
        scratch_shapes=[sem((2, n_j))],
        compiler_params=pltpu.CompilerParams(vmem_limit_bytes=1024 * 1024),
    )(standardized, tracer_end)
    return standardized.reshape(shape), tracer_end.reshape(shape)


def solution(mesh):
    sizes = (mesh.shape["lat"], mesh.shape["lon"], mesh.shape["lev"])
    spec = P(("unit", "lat"), "lon", "lev", None)
    return jax.shard_map(
        functools.partial(on_device, sizes),
        mesh=mesh,
        in_specs=(spec, spec, spec),
        out_specs=(spec, spec),
        check_vma=False,
    )
```

```python
import functools

import jax
import jax.numpy as jnp
from jax import lax
from jax.experimental import pallas as pl
from jax.experimental.pallas import tpu as pltpu
from jax.sharding import PartitionSpec as P

STEPS = 4
PAD = 8
EPSILON = 0.0001
MESH = pl.DeviceIdType.MESH


def rows_of(extent):
    for rows in (32, 16, 8):
        if extent % rows == 0:
            return rows
    return extent


def others_near(extent):
    return sorted({1, extent - 1})


def steps_kernel(
    sizes, shape, tracer, diffusivity, source, last, tracer_end, own, others,
    field, coeff, forcing,
    load_sem, lev_send, lev_recv, lat_send, lat_recv, lon_send, lon_recv, stat_send, stat_recv,
):
    n_j, n_i, n_k, _ = shape
    n_lat, n_lon, n_lev = sizes
    inner = pl.ds(PAD, n_i)
    whole_j = pl.ds(1, n_j)
    chunk = rows_of(n_i)
    lat, lon, lev = lax.axis_index("lat"), lax.axis_index("lon"), lax.axis_index("lev")
    lat_up, lat_down = lax.rem(lat + 1, n_lat), lax.rem(lat + n_lat - 1, n_lat)
    lon_up, lon_down = lax.rem(lon + 1, n_lon), lax.rem(lon + n_lon - 1, n_lon)
    lev_up, lev_down = lax.rem(lev + 1, n_lev), lax.rem(lev + n_lev - 1, n_lev)

    def load(which, k, sem):
        array = (tracer, diffusivity, source)[which]
        if which == 0:
            target = field.at[0, k + 1, whole_j, inner, :]
        else:
            target = (coeff, forcing)[which - 1].at[k]
        return pltpu.make_async_copy(array.at[:, :, k, :], target, load_sem.at[sem])

    def wait_for(ref, sem):
        pltpu.make_async_copy(ref, ref, sem).wait()

    def remote(src, dst, send, recv, device):
        return pltpu.make_async_remote_copy(
            src_ref=src, dst_ref=dst, send_sem=send, recv_sem=recv,
            device_id=device, device_id_type=MESH,
        )

    def send_lev(step, j):
        recv = lev_recv.at[step % 2, j - 1]
        for edge, halo, to in ((1, n_k + 1, lev_down), (n_k, 0, lev_up)):
            src = field.at[step, edge, j, inner, :]
            remote(src, field.at[step, halo, j, inner, :], lev_send, recv, {"lev": to}).start()

    def wait_lev(step, j):
        wait_for(field.at[step, pl.ds(0, 2), j, inner, :], lev_recv.at[step % 2, j - 1])

    edges, middle = (pl.ds(1, 1), pl.ds(n_k, 1)), (pl.ds(2, n_k - 2),)

    def send_lat(step, planes, side):
        src, dst, to = ((1, n_j + 1, lat_down), (n_j, 0, lat_up))[side]
        recv = lat_recv.at[step % 2, len(planes) - 1]
        for k in planes:
            remote(
                field.at[step, k, src, inner, :], field.at[step, k, dst, inner, :],
                lat_send, recv, {"lat": to},
            ).start()

    def send_lon(step, planes):
        recv = lon_recv.at[step % 2, len(planes) - 1]
        for src, dst, to in ((PAD, PAD + n_i, lon_down), (PAD + n_i - 1, PAD - 1, lon_up)):
            for k in planes:
                remote(
                    field.at[step, k, whole_j, pl.ds(src, 1), :],
                    field.at[step, k, whole_j, pl.ds(dst, 1), :],
                    lon_send, recv, {"lon": to},
                ).start()

    def wait_sides(step, planes):
        count = 2 if len(planes) == 2 else n_k - 2
        k = pl.ds(1, count)
        wait_for(field.at[step, k, pl.ds(0, 2), inner, :], lat_recv.at[step % 2, len(planes) - 1])
        wait_for(
            field.at[step, k, whole_j, pl.ds(PAD, 2), :], lon_recv.at[step % 2, len(planes) - 1]
        )

    def stat_copies(j):
        return [
            remote(
                own.at[j - 1], others.at[n_lev - 1 - away, j - 1],
                stat_send, stat_recv.at[n_lev - 1 - away, j - 1],
                {"lev": lax.rem(lev + away, n_lev)},
            )
            for away in range(1, n_lev)
        ]

    def update(step, k, j):
        for low in range(0, n_i, chunk):
            r = PAD + low
            middle = field[step, k, j, pl.ds(r, chunk), :]
            spread = (
                field[step, k, j - 1, pl.ds(r, chunk), :] + field[step, k, j + 1, pl.ds(r, chunk), :]
                + field[step, k, j, pl.ds(r - 1, chunk), :] + field[step, k, j, pl.ds(r + 1, chunk), :]
                + field[step, k - 1, j, pl.ds(r, chunk), :] + field[step, k + 1, j, pl.ds(r, chunk), :]
                - 6.0 * middle
            )
            rows = pl.ds(low, chunk)
            value = middle + coeff[k - 1, j - 1, rows, :] * spread + forcing[k - 1, j - 1, rows, :]
            if step == STEPS - 1:
                last[k - 1, j - 1, rows, :] = value
                place = pl.ds(low * n_k + k - 1, chunk, stride=n_k)
                tracer_end[j - 1, place, :] = value
            else:
                field[step + 1, k, j, pl.ds(r, chunk), :] = value

    def summarise(j):
        for low in range(0, n_i, chunk):
            rows = pl.ds(low, chunk)
            total = last[0, j - 1, rows, :]
            for k in range(1, n_k):
                total = total + last[k, j - 1, rows, :]
            mean = total * (1.0 / n_k)
            squares = jnp.zeros_like(mean)
            for k in range(n_k):
                moved = last[k, j - 1, rows, :] - mean
                squares = squares + moved * moved
            own[j - 1, 0, rows, :] = mean
            own[j - 1, 1, rows, :] = squares

    def over_k(first, end, body):
        def wrapped(k, carry):
            body(k)
            return carry
        lax.fori_loop(first, end, wrapped, 0)

    for k in (0, n_k - 1):
        load(0, k, 3).start()

    barrier = pltpu.get_barrier_semaphore()

    def greet(axis, place, extent, sem):
        for away in others_near(extent):
            pl.semaphore_signal(
                sem, inc=1, device_id={axis: lax.rem(place + away, extent)}, device_id_type=MESH
            )

    greet("lat", lat, n_lat, barrier)
    greet("lon", lon, n_lon, barrier)
    for away in range(1, n_lev):
        pl.semaphore_signal(
            barrier, inc=1, device_id={"lev": lax.rem(lev + away, n_lev)}, device_id_type=MESH
        )
    expected = len(others_near(n_lat)) + len(others_near(n_lon)) + n_lev - 1
    with jax.named_scope("barrier"):
        pl.semaphore_wait(barrier, expected)
    with jax.named_scope("edges"):
        wait_for(field.at[0, pl.ds(1, 2), whole_j, inner, :], load_sem.at[3])
    for j in range(1, n_j + 1):
        send_lev(0, j)
    over_k(1, n_k - 1, lambda k: load(0, k, 0).start())
    for which in (1, 2):
        over_k(0, n_k, lambda k: load(which, k, which).start())
    for side in (0, 1):
        send_lat(0, edges, side)
    send_lon(0, edges)
    with jax.named_scope("load"):
        wait_for(field.at[0, pl.ds(1, n_k - 2), whole_j, inner, :], load_sem.at[0])
    for side in (0, 1):
        send_lat(0, middle, side)
    send_lon(0, middle)
    with jax.named_scope("load_rest"):
        wait_for(coeff, load_sem.at[1])
        wait_for(forcing, load_sem.at[2])

    def inside(step):
        with jax.named_scope(f"sides{step}"):
            wait_sides(step, middle)

        def body(k):
            def across(j, carry):
                update(step, k, j)
                return carry
            lax.fori_loop(1, n_j + 1, across, 0)

        with jax.named_scope(f"inside{step}"):
            over_k(2, n_k, body)
        if step < STEPS - 1:
            for side in (0, 1):
                send_lat(step + 1, middle, side)
            send_lon(step + 1, middle)

    def outside(step):
        with jax.named_scope(f"face_sides{step}"):
            wait_sides(step, edges)
        for j in range(1, n_j + 1):
            with jax.named_scope(f"lev{step}_{j}"):
                wait_lev(step, j)
            with jax.named_scope(f"face{step}_{j}"):
                update(step, 1, j)
                update(step, n_k, j)
            if step < STEPS - 1:
                send_lev(step + 1, j)
                for side, edge in ((0, 1), (1, n_j)):
                    if j == edge:
                        send_lat(step + 1, edges, side)
            else:
                with jax.named_scope(f"sum{j}"):
                    summarise(j)
                for copy in stat_copies(j):
                    copy.start()
        if step < STEPS - 1:
            send_lon(step + 1, edges)

    for step in range(STEPS):
        inside(step)
        outside(step)
    for j in range(1, n_j + 1):
        with jax.named_scope(f"stat{j}"):
            for copy in stat_copies(j):
                copy.wait_recv()
    with jax.named_scope("sent"):
        wait_for(field.at[:, pl.ds(0, 2), whole_j, inner, :], lev_send)
        wait_for(field.at[:, pl.ds(1, n_k), pl.ds(0, 2), inner, :], lat_send)
        wait_for(field.at[:, pl.ds(1, n_k), whole_j, pl.ds(PAD, 2), :], lon_send)
        wait_for(others, stat_send)


def finish_kernel(
    shape, n_lev, last, tracer_end, own, others, standardized_out, tracer_out, standardized, sem,
):
    n_j, n_i, n_k, _ = shape
    chunk = rows_of(n_i)

    def combine(j):
        for low in range(0, n_i, chunk):
            rows = pl.ds(low, chunk)
            means = [own[j - 1, 0, rows, :]] + [others[p, j - 1, 0, rows, :] for p in range(n_lev - 1)]
            mean = functools.reduce(jnp.add, means) * (1.0 / n_lev)
            squares = own[j - 1, 1, rows, :]
            for p in range(n_lev - 1):
                squares = squares + others[p, j - 1, 1, rows, :]
            for part in means:
                squares = squares + n_k * ((part - mean) * (part - mean))
            scale = lax.rsqrt(squares * (1.0 / (n_k * n_lev)) + EPSILON)
            for k in range(n_k):
                place = pl.ds(low * n_k + k, chunk, stride=n_k)
                standardized[j - 1, place, :] = (last[k, j - 1, rows, :] - mean) * scale

    def write(which, j):
        src, dst = ((tracer_end, tracer_out), (standardized, standardized_out))[which]
        return pltpu.make_async_copy(src.at[j], dst.at[j], sem.at[which, j])

    for j in range(n_j):
        write(0, j).start()
    for j in range(n_j):
        combine(j + 1)
        write(1, j).start()
    for which in (0, 1):
        for j in range(n_j):
            write(which, j).wait()


def on_device(sizes, tracer, diffusivity, source):
    shape = tracer.shape
    n_j, n_i, n_k, levels = shape
    n_lev = sizes[2]
    f32 = jnp.float32
    sem = pltpu.SemaphoreType.DMA
    flat = (n_j, n_i * n_k, levels)
    parts = (
        pltpu.VMEM((n_k, n_j, n_i, levels), f32),
        pltpu.VMEM(flat, f32),
        pltpu.VMEM((n_j, 2, n_i, levels), f32),
        pltpu.VMEM((n_lev - 1, n_j, 2, n_i, levels), f32),
    )
    results = pl.pallas_call(
        functools.partial(steps_kernel, sizes, shape),
        out_shape=parts,
        in_specs=[pl.BlockSpec(memory_space=pl.ANY)] * 3,
        out_specs=(pl.BlockSpec(memory_space=pltpu.VMEM),) * len(parts),
        scratch_shapes=[
            pltpu.VMEM((STEPS, n_k + 2, n_j + 2, n_i + 2 * PAD, levels), f32),
            pltpu.VMEM((n_k, n_j, n_i, levels), f32),
            pltpu.VMEM((n_k, n_j, n_i, levels), f32),
            sem((4,)),
            sem, sem((2, n_j)),
            sem, sem((2, 2)),
            sem, sem((2, 2)),
            sem, sem((n_lev - 1, n_j)),
        ],
        compiler_params=pltpu.CompilerParams(
            collective_id=0, has_side_effects=True, vmem_limit_bytes=48 * 1024 * 1024,
        ),
    )(tracer, diffusivity, source)
    standardized, tracer_end = pl.pallas_call(
        functools.partial(finish_kernel, shape, n_lev),
        out_shape=(jax.ShapeDtypeStruct(flat, f32),) * 2,
        in_specs=[pl.BlockSpec(memory_space=pltpu.VMEM)] * len(parts),
        out_specs=(pl.BlockSpec(memory_space=pl.ANY),) * 2,
        scratch_shapes=[pltpu.VMEM(flat, f32), sem((2, n_j))],
        compiler_params=pltpu.CompilerParams(vmem_limit_bytes=8 * 1024 * 1024),
    )(*results)
    return standardized.reshape(shape), tracer_end.reshape(shape)


def solution(mesh):
    sizes = (mesh.shape["lat"], mesh.shape["lon"], mesh.shape["lev"])
    spec = P(("unit", "lat"), "lon", "lev", None)
    return jax.shard_map(
        functools.partial(on_device, sizes),
        mesh=mesh,
        in_specs=(spec, spec, spec),
        out_specs=(spec, spec),
        check_vma=False,
    )
```

```python
import functools

import jax
import jax.numpy as jnp
from jax import lax
from jax.experimental import pallas as pl
from jax.experimental.pallas import tpu as pltpu
from jax.sharding import PartitionSpec as P

STEPS = 4
PAD = 8
EPSILON = 0.0001
MESH = pl.DeviceIdType.MESH


def rows_of(extent):
    for rows in (32, 16, 8):
        if extent % rows == 0:
            return rows
    return extent


def others_near(extent):
    return sorted({1, extent - 1})


def steps_kernel(
    sizes, shape, tracer, diffusivity, source, last, tracer_end, own, others,
    field, coeff, forcing,
    load_sem, lev_send, lev_recv, lat_send, lat_recv, lon_send, lon_recv, stat_send, stat_recv, ready,
):
    n_j, n_i, n_k, _ = shape
    n_lat, n_lon, n_lev = sizes
    inner = pl.ds(PAD, n_i)
    whole_j = pl.ds(1, n_j)
    chunk = rows_of(n_i)
    lat, lon, lev = lax.axis_index("lat"), lax.axis_index("lon"), lax.axis_index("lev")
    lat_up, lat_down = lax.rem(lat + 1, n_lat), lax.rem(lat + n_lat - 1, n_lat)
    lon_up, lon_down = lax.rem(lon + 1, n_lon), lax.rem(lon + n_lon - 1, n_lon)
    lev_up, lev_down = lax.rem(lev + 1, n_lev), lax.rem(lev + n_lev - 1, n_lev)

    def load(which, k, sem):
        array = (tracer, diffusivity, source)[which]
        if which == 0:
            target = field.at[0, k + 1, whole_j, inner, :]
        else:
            target = (coeff, forcing)[which - 1].at[k]
        return pltpu.make_async_copy(array.at[:, :, k, :], target, load_sem.at[sem])

    def load_edge(j, k):
        return pltpu.make_async_copy(
            tracer.at[j - 1, :, k, :], field.at[0, k + 1, j, inner, :], load_sem.at[2 + j]
        )

    def wait_for(ref, sem):
        pltpu.make_async_copy(ref, ref, sem).wait()

    def remote(src, dst, send, recv, device):
        return pltpu.make_async_remote_copy(
            src_ref=src, dst_ref=dst, send_sem=send, recv_sem=recv,
            device_id=device, device_id_type=MESH,
        )

    def send_lev(step, j):
        recv = lev_recv.at[step % 2, j - 1]
        for edge, halo, to in ((1, n_k + 1, lev_down), (n_k, 0, lev_up)):
            src = field.at[step, edge, j, inner, :]
            remote(src, field.at[step, halo, j, inner, :], lev_send, recv, {"lev": to}).start()

    def wait_lev(step, j):
        wait_for(field.at[step, pl.ds(0, 2), j, inner, :], lev_recv.at[step % 2, j - 1])

    edges, middle = (pl.ds(1, 1), pl.ds(n_k, 1)), (pl.ds(2, n_k - 2),)

    def send_lat(step, planes, side):
        src, dst, to = ((1, n_j + 1, lat_down), (n_j, 0, lat_up))[side]
        recv = lat_recv.at[step % 2, len(planes) - 1]
        for k in planes:
            remote(
                field.at[step, k, src, inner, :], field.at[step, k, dst, inner, :],
                lat_send, recv, {"lat": to},
            ).start()

    def send_lon(step, planes):
        recv = lon_recv.at[step % 2, len(planes) - 1]
        for src, dst, to in ((PAD, PAD + n_i, lon_down), (PAD + n_i - 1, PAD - 1, lon_up)):
            for k in planes:
                remote(
                    field.at[step, k, whole_j, pl.ds(src, 1), :],
                    field.at[step, k, whole_j, pl.ds(dst, 1), :],
                    lon_send, recv, {"lon": to},
                ).start()

    def wait_sides(step, planes):
        count = 2 if len(planes) == 2 else n_k - 2
        k = pl.ds(1, count)
        wait_for(field.at[step, k, pl.ds(0, 2), inner, :], lat_recv.at[step % 2, len(planes) - 1])
        wait_for(
            field.at[step, k, whole_j, pl.ds(PAD, 2), :], lon_recv.at[step % 2, len(planes) - 1]
        )

    def stat_copies(j):
        return [
            remote(
                own.at[j - 1], others.at[n_lev - 1 - away, j - 1],
                stat_send, stat_recv.at[n_lev - 1 - away, j - 1],
                {"lev": lax.rem(lev + away, n_lev)},
            )
            for away in range(1, n_lev)
        ]

    def update(step, k, j):
        for low in range(0, n_i, chunk):
            r = PAD + low
            middle = field[step, k, j, pl.ds(r, chunk), :]
            spread = (
                field[step, k, j - 1, pl.ds(r, chunk), :] + field[step, k, j + 1, pl.ds(r, chunk), :]
                + field[step, k, j, pl.ds(r - 1, chunk), :] + field[step, k, j, pl.ds(r + 1, chunk), :]
                + field[step, k - 1, j, pl.ds(r, chunk), :] + field[step, k + 1, j, pl.ds(r, chunk), :]
                - 6.0 * middle
            )
            rows = pl.ds(low, chunk)
            value = middle + coeff[k - 1, j - 1, rows, :] * spread + forcing[k - 1, j - 1, rows, :]
            if step == STEPS - 1:
                last[k - 1, j - 1, rows, :] = value
                place = pl.ds(low * n_k + k - 1, chunk, stride=n_k)
                tracer_end[j - 1, place, :] = value
            else:
                field[step + 1, k, j, pl.ds(r, chunk), :] = value

    def summarise(j):
        for low in range(0, n_i, chunk):
            rows = pl.ds(low, chunk)
            total = last[0, j - 1, rows, :]
            for k in range(1, n_k):
                total = total + last[k, j - 1, rows, :]
            mean = total * (1.0 / n_k)
            squares = jnp.zeros_like(mean)
            for k in range(n_k):
                moved = last[k, j - 1, rows, :] - mean
                squares = squares + moved * moved
            own[j - 1, 0, rows, :] = mean
            own[j - 1, 1, rows, :] = squares

    def over_k(first, end, body):
        def wrapped(k, carry):
            body(k)
            return carry
        lax.fori_loop(first, end, wrapped, 0)

    for j in range(1, n_j + 1):
        for k in (0, n_k - 1):
            load_edge(j, k).start()

    barrier = pltpu.get_barrier_semaphore()

    def greet(axis, place, extent, sem):
        for away in others_near(extent):
            pl.semaphore_signal(
                sem, inc=1, device_id={axis: lax.rem(place + away, extent)}, device_id_type=MESH
            )

    sides = (("lat", lat, n_lat), ("lon", lon, n_lon))
    pairs = [extent % 2 == 0 for _, _, extent in sides]
    expected = n_lev - 1
    for away in range(1, n_lev):
        pl.semaphore_signal(
            barrier, inc=1, device_id={"lev": lax.rem(lev + away, n_lev)}, device_id_type=MESH
        )
    for paired, (axis, place, extent) in zip(pairs, sides):
        if paired:
            pl.when(lax.rem(place, 2) == 0)(functools.partial(greet, axis, place, extent, barrier))
            expected = expected + lax.rem(place, 2) * len(others_near(extent))
        else:
            greet(axis, place, extent, barrier)
            expected = expected + len(others_near(extent))
    with jax.named_scope("barrier"):
        pl.semaphore_wait(barrier, expected)
    for j in range(1, n_j + 1):
        wait_for(field.at[0, pl.ds(1, 2), j, inner, :], load_sem.at[2 + j])
        send_lev(0, j)
    over_k(1, n_k - 1, lambda k: load(0, k, 0).start())
    for which in (1, 2):
        over_k(0, n_k, lambda k: load(which, k, which).start())
    for n, (paired, (axis, place, extent)) in enumerate(zip(pairs, sides)):
        if paired:
            @pl.when(lax.rem(place, 2) == 1)
            def _():
                greet(axis, place, extent, ready.at[n])

            @pl.when(lax.rem(place, 2) == 0)
            def _():
                pl.semaphore_wait(ready.at[n], len(others_near(extent)))

    for side in (0, 1):
        send_lat(0, edges, side)
    send_lon(0, edges)
    with jax.named_scope("load"):
        wait_for(field.at[0, pl.ds(1, n_k - 2), whole_j, inner, :], load_sem.at[0])
    for side in (0, 1):
        send_lat(0, middle, side)
    send_lon(0, middle)
    with jax.named_scope("load_rest"):
        wait_for(coeff, load_sem.at[1])
        wait_for(forcing, load_sem.at[2])

    def inside(step):
        with jax.named_scope(f"sides{step}"):
            wait_sides(step, middle)

        def body(k):
            def across(j, carry):
                update(step, k, j)
                return carry
            lax.fori_loop(1, n_j + 1, across, 0)

        with jax.named_scope(f"inside{step}"):
            over_k(2, n_k, body)
        if step < STEPS - 1:
            for side in (0, 1):
                send_lat(step + 1, middle, side)
            send_lon(step + 1, middle)

    def outside(step):
        with jax.named_scope(f"face_sides{step}"):
            wait_sides(step, edges)
        for j in range(1, n_j + 1):
            with jax.named_scope(f"lev{step}_{j}"):
                wait_lev(step, j)
            with jax.named_scope(f"face{step}_{j}"):
                update(step, 1, j)
                update(step, n_k, j)
            if step < STEPS - 1:
                send_lev(step + 1, j)
                for side, edge in ((0, 1), (1, n_j)):
                    if j == edge:
                        send_lat(step + 1, edges, side)
            else:
                with jax.named_scope(f"sum{j}"):
                    summarise(j)
                for copy in stat_copies(j):
                    copy.start()
        if step < STEPS - 1:
            send_lon(step + 1, edges)

    for step in range(STEPS):
        inside(step)
        outside(step)
    for j in range(1, n_j + 1):
        with jax.named_scope(f"stat{j}"):
            for copy in stat_copies(j):
                copy.wait_recv()
    with jax.named_scope("sent"):
        wait_for(field.at[:, pl.ds(0, 2), whole_j, inner, :], lev_send)
        wait_for(field.at[:, pl.ds(1, n_k), pl.ds(0, 2), inner, :], lat_send)
        wait_for(field.at[:, pl.ds(1, n_k), whole_j, pl.ds(PAD, 2), :], lon_send)
        wait_for(others, stat_send)


def finish_kernel(
    shape, n_lev, last, tracer_end, own, others, standardized_out, tracer_out, standardized, sem,
):
    n_j, n_i, n_k, _ = shape
    chunk = rows_of(n_i)

    def combine(j):
        for low in range(0, n_i, chunk):
            rows = pl.ds(low, chunk)
            means = [own[j - 1, 0, rows, :]] + [others[p, j - 1, 0, rows, :] for p in range(n_lev - 1)]
            mean = functools.reduce(jnp.add, means) * (1.0 / n_lev)
            squares = own[j - 1, 1, rows, :]
            for p in range(n_lev - 1):
                squares = squares + others[p, j - 1, 1, rows, :]
            for part in means:
                squares = squares + n_k * ((part - mean) * (part - mean))
            scale = lax.rsqrt(squares * (1.0 / (n_k * n_lev)) + EPSILON)
            for k in range(n_k):
                place = pl.ds(low * n_k + k, chunk, stride=n_k)
                standardized[j - 1, place, :] = (last[k, j - 1, rows, :] - mean) * scale

    def write(which, j):
        src, dst = ((tracer_end, tracer_out), (standardized, standardized_out))[which]
        return pltpu.make_async_copy(src.at[j], dst.at[j], sem.at[which, j])

    for j in range(n_j):
        write(0, j).start()
    for j in range(n_j):
        combine(j + 1)
        write(1, j).start()
    for which in (0, 1):
        for j in range(n_j):
            write(which, j).wait()


def on_device(sizes, tracer, diffusivity, source):
    shape = tracer.shape
    n_j, n_i, n_k, levels = shape
    n_lev = sizes[2]
    f32 = jnp.float32
    sem = pltpu.SemaphoreType.DMA
    flat = (n_j, n_i * n_k, levels)
    parts = (
        pltpu.VMEM((n_k, n_j, n_i, levels), f32),
        pltpu.VMEM(flat, f32),
        pltpu.VMEM((n_j, 2, n_i, levels), f32),
        pltpu.VMEM((n_lev - 1, n_j, 2, n_i, levels), f32),
    )
    results = pl.pallas_call(
        functools.partial(steps_kernel, sizes, shape),
        out_shape=parts,
        in_specs=[pl.BlockSpec(memory_space=pl.ANY)] * 3,
        out_specs=(pl.BlockSpec(memory_space=pltpu.VMEM),) * len(parts),
        scratch_shapes=[
            pltpu.VMEM((STEPS, n_k + 2, n_j + 2, n_i + 2 * PAD, levels), f32),
            pltpu.VMEM((n_k, n_j, n_i, levels), f32),
            pltpu.VMEM((n_k, n_j, n_i, levels), f32),
            sem((n_j + 3,)),
            sem, sem((2, n_j)),
            sem, sem((2, 2)),
            sem, sem((2, 2)),
            sem, sem((n_lev - 1, n_j)),
            pltpu.SemaphoreType.REGULAR((2,)),
        ],
        compiler_params=pltpu.CompilerParams(
            collective_id=0, has_side_effects=True, vmem_limit_bytes=48 * 1024 * 1024,
        ),
    )(tracer, diffusivity, source)
    standardized, tracer_end = pl.pallas_call(
        functools.partial(finish_kernel, shape, n_lev),
        out_shape=(jax.ShapeDtypeStruct(flat, f32),) * 2,
        in_specs=[pl.BlockSpec(memory_space=pltpu.VMEM)] * len(parts),
        out_specs=(pl.BlockSpec(memory_space=pl.ANY),) * 2,
        scratch_shapes=[pltpu.VMEM(flat, f32), sem((2, n_j))],
        compiler_params=pltpu.CompilerParams(vmem_limit_bytes=8 * 1024 * 1024),
    )(*results)
    return standardized.reshape(shape), tracer_end.reshape(shape)


def solution(mesh):
    sizes = (mesh.shape["lat"], mesh.shape["lon"], mesh.shape["lev"])
    spec = P(("unit", "lat"), "lon", "lev", None)
    return jax.shard_map(
        functools.partial(on_device, sizes),
        mesh=mesh,
        in_specs=(spec, spec, spec),
        out_specs=(spec, spec),
        check_vma=False,
    )
```

```python
import functools

import jax
import jax.numpy as jnp
from jax import lax
from jax.experimental import pallas as pl
from jax.experimental.pallas import tpu as pltpu
from jax.sharding import PartitionSpec as P

STEPS = 4
PAD = 8
EPSILON = 0.0001
MESH = pl.DeviceIdType.MESH


def rows_of(extent):
    for rows in (32, 16, 8):
        if extent % rows == 0:
            return rows
    return extent


def others_near(extent):
    return sorted({1, extent - 1})


def steps_kernel(
    sizes, shape, tracer, diffusivity, source, last, tracer_end, own, others,
    field, coeff, forcing,
    load_sem, lev_send, lev_recv, lat_send, lat_recv, lon_send, lon_recv, stat_send, stat_recv, ready,
):
    n_j, n_i, n_k, _ = shape
    n_lat, n_lon, n_lev = sizes
    inner = pl.ds(PAD, n_i)
    whole_j = pl.ds(1, n_j)
    chunk = rows_of(n_i)
    lat, lon, lev = lax.axis_index("lat"), lax.axis_index("lon"), lax.axis_index("lev")
    lat_up, lat_down = lax.rem(lat + 1, n_lat), lax.rem(lat + n_lat - 1, n_lat)
    lon_up, lon_down = lax.rem(lon + 1, n_lon), lax.rem(lon + n_lon - 1, n_lon)
    lev_up, lev_down = lax.rem(lev + 1, n_lev), lax.rem(lev + n_lev - 1, n_lev)

    first_half = lax.rem(lat, 2) == 0

    def load(which, k, sem):
        array = (tracer, diffusivity, source)[which]
        if which == 0:
            target = field.at[0, k + 1, whole_j, inner, :]
        else:
            target = (coeff, forcing)[which - 1].at[k]
        return pltpu.make_async_copy(array.at[:, :, k, :], target, load_sem.at[sem])

    def load_edge(j, k):
        return pltpu.make_async_copy(
            tracer.at[j - 1, :, k, :], field.at[0, k + 1, j, inner, :], load_sem.at[2 + j]
        )

    def wait_for(ref, sem):
        pltpu.make_async_copy(ref, ref, sem).wait()

    def remote(src, dst, send, recv, device):
        return pltpu.make_async_remote_copy(
            src_ref=src, dst_ref=dst, send_sem=send, recv_sem=recv,
            device_id=device, device_id_type=MESH,
        )

    def send_lev(step, j):
        recv = lev_recv.at[step % 2, j - 1]
        for edge, halo, to in ((1, n_k + 1, lev_down), (n_k, 0, lev_up)):
            src = field.at[step, edge, j, inner, :]
            remote(src, field.at[step, halo, j, inner, :], lev_send, recv, {"lev": to}).start()

    def wait_lev(step, j):
        wait_for(field.at[step, pl.ds(0, 2), j, inner, :], lev_recv.at[step % 2, j - 1])

    edges, middle = (pl.ds(1, 1), pl.ds(n_k, 1)), (pl.ds(2, n_k - 2),)

    def send_lat(step, planes, side):
        src, dst, to = ((1, n_j + 1, lat_down), (n_j, 0, lat_up))[side]
        recv = lat_recv.at[step % 2, len(planes) - 1]
        for k in planes:
            remote(
                field.at[step, k, src, inner, :], field.at[step, k, dst, inner, :],
                lat_send, recv, {"lat": to},
            ).start()

    def send_lon(step, planes):
        recv = lon_recv.at[step % 2, len(planes) - 1]
        for src, dst, to in ((PAD, PAD + n_i, lon_down), (PAD + n_i - 1, PAD - 1, lon_up)):
            for k in planes:
                remote(
                    field.at[step, k, whole_j, pl.ds(src, 1), :],
                    field.at[step, k, whole_j, pl.ds(dst, 1), :],
                    lon_send, recv, {"lon": to},
                ).start()

    def wait_sides(step, planes):
        count = 2 if len(planes) == 2 else n_k - 2
        k = pl.ds(1, count)
        wait_for(field.at[step, k, pl.ds(0, 2), inner, :], lat_recv.at[step % 2, len(planes) - 1])
        wait_for(
            field.at[step, k, whole_j, pl.ds(PAD, 2), :], lon_recv.at[step % 2, len(planes) - 1]
        )

    def stat_copies(j):
        return [
            remote(
                own.at[j - 1], others.at[n_lev - 1 - away, j - 1],
                stat_send, stat_recv.at[n_lev - 1 - away, j - 1],
                {"lev": lax.rem(lev + away, n_lev)},
            )
            for away in range(1, n_lev)
        ]

    def update(step, k, j):
        for low in range(0, n_i, chunk):
            r = PAD + low
            middle = field[step, k, j, pl.ds(r, chunk), :]
            spread = (
                field[step, k, j - 1, pl.ds(r, chunk), :] + field[step, k, j + 1, pl.ds(r, chunk), :]
                + field[step, k, j, pl.ds(r - 1, chunk), :] + field[step, k, j, pl.ds(r + 1, chunk), :]
                + field[step, k - 1, j, pl.ds(r, chunk), :] + field[step, k + 1, j, pl.ds(r, chunk), :]
                - 6.0 * middle
            )
            rows = pl.ds(low, chunk)
            value = middle + coeff[k - 1, j - 1, rows, :] * spread + forcing[k - 1, j - 1, rows, :]
            if step == STEPS - 1:
                last[k - 1, j - 1, rows, :] = value
                place = pl.ds(low * n_k + k - 1, chunk, stride=n_k)
                tracer_end[j - 1, place, :] = value
            else:
                field[step + 1, k, j, pl.ds(r, chunk), :] = value

    def summarise(j):
        for low in range(0, n_i, chunk):
            rows = pl.ds(low, chunk)
            total = last[0, j - 1, rows, :]
            for k in range(1, n_k):
                total = total + last[k, j - 1, rows, :]
            mean = total * (1.0 / n_k)
            squares = jnp.zeros_like(mean)
            for k in range(n_k):
                moved = last[k, j - 1, rows, :] - mean
                squares = squares + moved * moved
            own[j - 1, 0, rows, :] = mean
            own[j - 1, 1, rows, :] = squares

    def over_k(first, end, body):
        def wrapped(k, carry):
            body(k)
            return carry
        lax.fori_loop(first, end, wrapped, 0)

    for j in range(1, n_j + 1):
        for k in (0, n_k - 1):
            load_edge(j, k).start()

    barrier = pltpu.get_barrier_semaphore()

    def greet(axis, place, extent, sem):
        for away in others_near(extent):
            pl.semaphore_signal(
                sem, inc=1, device_id={axis: lax.rem(place + away, extent)}, device_id_type=MESH
            )

    sides = (("lat", lat, n_lat), ("lon", lon, n_lon))
    pairs = [extent % 2 == 0 for _, _, extent in sides]
    expected = n_lev - 1
    for away in range(1, n_lev):
        pl.semaphore_signal(
            barrier, inc=1, device_id={"lev": lax.rem(lev + away, n_lev)}, device_id_type=MESH
        )
    for paired, (axis, place, extent) in zip(pairs, sides):
        if paired:
            pl.when(lax.rem(place, 2) == 0)(functools.partial(greet, axis, place, extent, barrier))
            expected = expected + lax.rem(place, 2) * len(others_near(extent))
        else:
            greet(axis, place, extent, barrier)
            expected = expected + len(others_near(extent))
    with jax.named_scope("barrier"):
        pl.semaphore_wait(barrier, expected)
    for j in range(1, n_j + 1):
        wait_for(field.at[0, pl.ds(1, 2), j, inner, :], load_sem.at[2 + j])
        send_lev(0, j)
    over_k(1, n_k - 1, lambda k: load(0, k, 0).start())
    for which in (1, 2):
        over_k(0, n_k, lambda k: load(which, k, which).start())
    for n, (paired, (axis, place, extent)) in enumerate(zip(pairs, sides)):
        if paired:
            @pl.when(lax.rem(place, 2) == 1)
            def _():
                greet(axis, place, extent, ready.at[n])

            @pl.when(lax.rem(place, 2) == 0)
            def _():
                pl.semaphore_wait(ready.at[n], len(others_near(extent)))

    for side in (0, 1):
        send_lat(0, edges, side)
    send_lon(0, edges)
    with jax.named_scope("load"):
        wait_for(field.at[0, pl.ds(1, n_k - 2), whole_j, inner, :], load_sem.at[0])
    for side in (0, 1):
        send_lat(0, middle, side)
    send_lon(0, middle)
    with jax.named_scope("load_rest"):
        wait_for(coeff, load_sem.at[1])
        wait_for(forcing, load_sem.at[2])

    def inside(step):
        with jax.named_scope(f"sides{step}"):
            wait_sides(step, middle)

        def body(k):
            def across(j, carry):
                update(step, k, j)
                return carry
            lax.fori_loop(1, n_j + 1, across, 0)

        with jax.named_scope(f"inside{step}"):
            over_k(2, n_k, body)
        if step < STEPS - 1:
            for side in (0, 1):
                send_lat(step + 1, middle, side)
            send_lon(step + 1, middle)

    def outside(step):
        with jax.named_scope(f"face_sides{step}"):
            wait_sides(step, edges)
        for j in range(1, n_j + 1):
            with jax.named_scope(f"lev{step}_{j}"):
                wait_lev(step, j)
            with jax.named_scope(f"face{step}_{j}"):
                update(step, 1, j)
                update(step, n_k, j)
            if step < STEPS - 1:
                send_lev(step + 1, j)
                for side, edge in ((0, 1), (1, n_j)):
                    if j == edge:
                        send_lat(step + 1, edges, side)
            else:
                with jax.named_scope(f"sum{j}"):
                    summarise(j)
                @pl.when(first_half)
                def _():
                    for copy in stat_copies(j):
                        copy.start()
        if step < STEPS - 1:
            send_lon(step + 1, edges)

    for step in range(STEPS):
        inside(step)
        outside(step)

    @pl.when(first_half)
    def _():
        for j in range(1, n_j + 1):
            with jax.named_scope(f"stat{j}"):
                for copy in stat_copies(j):
                    copy.wait_recv()
        wait_for(others, stat_send)

    with jax.named_scope("sent"):
        wait_for(field.at[:, pl.ds(0, 2), whole_j, inner, :], lev_send)
        wait_for(field.at[:, pl.ds(1, n_k), pl.ds(0, 2), inner, :], lat_send)
        wait_for(field.at[:, pl.ds(1, n_k), whole_j, pl.ds(PAD, 2), :], lon_send)


def combine(shape, n_lev, j, last, own, others, place_of):
    n_j, n_i, n_k, _ = shape
    chunk = rows_of(n_i)
    for low in range(0, n_i, chunk):
        rows = pl.ds(low, chunk)
        means = [own[j, 0, rows, :]] + [others[p, j, 0, rows, :] for p in range(n_lev - 1)]
        mean = functools.reduce(jnp.add, means) * (1.0 / n_lev)
        squares = own[j, 1, rows, :]
        for p in range(n_lev - 1):
            squares = squares + others[p, j, 1, rows, :]
        for part in means:
            squares = squares + n_k * ((part - mean) * (part - mean))
        scale = lax.rsqrt(squares * (1.0 / (n_k * n_lev)) + EPSILON)
        for k in range(n_k):
            place = pl.ds(low * n_k + k, chunk, stride=n_k)
            place_of[place, :] = (last[k, j, rows, :] - mean) * scale


def write_tracer(tracer_end, out, token, sem):
    copies = [
        pltpu.make_async_copy(tracer_end.at[j], out.at[j], sem.at[j])
        for j in range(tracer_end.shape[0])
    ]
    for copy in copies:
        copy.start()
    token[...] = jnp.zeros_like(token)
    for copy in copies:
        copy.wait()


def second_kernel(
    sizes, shape, last, own, early, token, others, standardized, send_sem, recv_sem,
):
    n_j, n_i, _, _ = shape
    n_lev = sizes[2]
    lat, lev = lax.axis_index("lat"), lax.axis_index("lev")
    second_half = lax.rem(lat, 2) == 1

    def copies(j):
        return [
            pltpu.make_async_remote_copy(
                src_ref=own.at[j], dst_ref=others.at[n_lev - 1 - away, j],
                send_sem=send_sem, recv_sem=recv_sem.at[n_lev - 1 - away, j],
                device_id={"lev": lax.rem(lev + away, n_lev)}, device_id_type=MESH,
            )
            for away in range(1, n_lev)
        ]

    @pl.when(second_half)
    def _():
        barrier = pltpu.get_barrier_semaphore()
        for away in range(1, n_lev):
            pl.semaphore_signal(
                barrier, inc=1, device_id={"lev": lax.rem(lev + away, n_lev)}, device_id_type=MESH
            )
        with jax.named_scope("barrier2"):
            pl.semaphore_wait(barrier, n_lev - 1)
        for j in range(n_j):
            for copy in copies(j):
                copy.start()

    @pl.when(lax.rem(lat, 2) == 0)
    def _():
        others[...] = early[...]

    for j in range(n_j):
        @pl.when(second_half)
        def _():
            with jax.named_scope(f"late{j}"):
                for copy in copies(j):
                    copy.wait_recv()

        if j < n_j - 1:
            combine(shape, n_lev, j, last, own, others, standardized.at[j])

    @pl.when(second_half)
    def _():
        pltpu.make_async_copy(others, others, send_sem).wait()


def finish_kernel(shape, n_lev, last, own, others, ready, out, final, sem):
    n_j = shape[0]
    copies = [
        pltpu.make_async_copy(final if j == n_j - 1 else ready.at[j], out.at[j], sem.at[j])
        for j in range(n_j)
    ]
    for copy in copies[:-1]:
        copy.start()
    combine(shape, n_lev, n_j - 1, last, own, others, final)
    copies[-1].start()
    for copy in copies:
        copy.wait()


def on_device(sizes, tracer, diffusivity, source):
    shape = tracer.shape
    n_j, n_i, n_k, levels = shape
    n_lev = sizes[2]
    f32 = jnp.float32
    sem = pltpu.SemaphoreType.DMA
    flat = (n_j, n_i * n_k, levels)
    parts = (
        pltpu.VMEM((n_k, n_j, n_i, levels), f32),
        pltpu.VMEM(flat, f32),
        pltpu.VMEM((n_j, 2, n_i, levels), f32),
        pltpu.VMEM((n_lev - 1, n_j, 2, n_i, levels), f32),
    )
    last, tracer_end, own, early = pl.pallas_call(
        functools.partial(steps_kernel, sizes, shape),
        out_shape=parts,
        in_specs=[pl.BlockSpec(memory_space=pl.ANY)] * 3,
        out_specs=(pl.BlockSpec(memory_space=pltpu.VMEM),) * len(parts),
        scratch_shapes=[
            pltpu.VMEM((STEPS, n_k + 2, n_j + 2, n_i + 2 * PAD, levels), f32),
            pltpu.VMEM((n_k, n_j, n_i, levels), f32),
            pltpu.VMEM((n_k, n_j, n_i, levels), f32),
            sem((n_j + 3,)),
            sem, sem((2, n_j)),
            sem, sem((2, 2)),
            sem, sem((2, 2)),
            sem, sem((n_lev - 1, n_j)),
            pltpu.SemaphoreType.REGULAR((2,)),
        ],
        compiler_params=pltpu.CompilerParams(
            collective_id=0, has_side_effects=True, vmem_limit_bytes=48 * 1024 * 1024,
        ),
    )(tracer, diffusivity, source)
    in_vmem, in_hbm = pl.BlockSpec(memory_space=pltpu.VMEM), pl.BlockSpec(memory_space=pl.ANY)
    tracer_end, token = pl.pallas_call(
        write_tracer,
        out_shape=(jax.ShapeDtypeStruct(flat, f32), pltpu.VMEM((8, levels), f32)),
        in_specs=[in_vmem],
        out_specs=(in_hbm, in_vmem),
        scratch_shapes=[sem((n_j,))],
        compiler_params=pltpu.CompilerParams(vmem_limit_bytes=1024 * 1024),
    )(tracer_end)
    others, standardized = pl.pallas_call(
        functools.partial(second_kernel, sizes, shape),
        out_shape=(parts[3], pltpu.VMEM(flat, f32)),
        in_specs=[in_vmem] * 4,
        out_specs=(in_vmem,) * 2,
        scratch_shapes=[sem, sem((n_lev - 1, n_j))],
        compiler_params=pltpu.CompilerParams(
            collective_id=1, has_side_effects=True, vmem_limit_bytes=8 * 1024 * 1024,
        ),
    )(last, own, early, token)
    standardized = pl.pallas_call(
        functools.partial(finish_kernel, shape, n_lev),
        out_shape=jax.ShapeDtypeStruct(flat, f32),
        in_specs=[in_vmem] * 4,
        out_specs=in_hbm,
        scratch_shapes=[pltpu.VMEM(flat[1:], f32), sem((n_j,))],
        compiler_params=pltpu.CompilerParams(vmem_limit_bytes=4 * 1024 * 1024),
    )(last, own, others, standardized)
    return standardized.reshape(shape), tracer_end.reshape(shape)


def solution(mesh):
    sizes = (mesh.shape["lat"], mesh.shape["lon"], mesh.shape["lev"])
    spec = P(("unit", "lat"), "lon", "lev", None)
    return jax.shard_map(
        functools.partial(on_device, sizes),
        mesh=mesh,
        in_specs=(spec, spec, spec),
        out_specs=(spec, spec),
        check_vma=False,
    )
```

```python
import functools

import jax
import jax.numpy as jnp
from jax import lax
from jax.experimental import pallas as pl
from jax.experimental.pallas import tpu as pltpu
from jax.sharding import PartitionSpec as P

STEPS = 4
PAD = 8
EPSILON = 0.0001
MESH = pl.DeviceIdType.MESH


def rows_of(extent):
    for rows in (32, 16, 8):
        if extent % rows == 0:
            return rows
    return extent


def others_near(extent):
    return sorted({1, extent - 1})


def steps_kernel(
    sizes, shape, tracer, diffusivity, source, last, tracer_end, own, others,
    field, coeff, forcing,
    load_sem, lev_send, lev_recv, lat_send, lat_recv, lon_send, lon_recv, stat_send, stat_recv, ready,
):
    n_j, n_i, n_k, _ = shape
    n_lat, n_lon, n_lev = sizes
    inner = pl.ds(PAD, n_i)
    whole_j = pl.ds(1, n_j)
    chunk = rows_of(n_i)
    lat, lon, lev = lax.axis_index("lat"), lax.axis_index("lon"), lax.axis_index("lev")
    lat_up, lat_down = lax.rem(lat + 1, n_lat), lax.rem(lat + n_lat - 1, n_lat)
    lon_up, lon_down = lax.rem(lon + 1, n_lon), lax.rem(lon + n_lon - 1, n_lon)
    lev_up, lev_down = lax.rem(lev + 1, n_lev), lax.rem(lev + n_lev - 1, n_lev)

    first_half = lax.rem(lat, 2) == 0

    def load(which, k, sem):
        array = (tracer, diffusivity, source)[which]
        if which == 0:
            target = field.at[0, k + 1, whole_j, inner, :]
        else:
            target = (coeff, forcing)[which - 1].at[k]
        return pltpu.make_async_copy(array.at[:, :, k, :], target, load_sem.at[sem])

    first = chunk if n_i > chunk else n_i

    def pieces(j):
        if j > 1 or first == n_i:
            return ((0, n_i),)
        return ((0, first), (first, n_i - first))

    def load_edge(j, k, piece):
        low, size = piece
        sem = 3 + n_j if (j == 1 and low > 0) else 2 + j
        return pltpu.make_async_copy(
            tracer.at[j - 1, pl.ds(low, size), k, :],
            field.at[0, k + 1, j, pl.ds(PAD + low, size), :], load_sem.at[sem],
        )

    def wait_for(ref, sem):
        pltpu.make_async_copy(ref, ref, sem).wait()

    def remote(src, dst, send, recv, device):
        return pltpu.make_async_remote_copy(
            src_ref=src, dst_ref=dst, send_sem=send, recv_sem=recv,
            device_id=device, device_id_type=MESH,
        )

    def send_lev(step, j, piece=None):
        low, size = piece or (0, n_i)
        rows = pl.ds(PAD + low, size)
        recv = lev_recv.at[step % 2, j - 1]
        for edge, halo, to in ((1, n_k + 1, lev_down), (n_k, 0, lev_up)):
            src = field.at[step, edge, j, rows, :]
            remote(src, field.at[step, halo, j, rows, :], lev_send, recv, {"lev": to}).start()

    def wait_lev(step, j):
        wait_for(field.at[step, pl.ds(0, 2), j, inner, :], lev_recv.at[step % 2, j - 1])

    edges, middle = (pl.ds(1, 1), pl.ds(n_k, 1)), (pl.ds(2, n_k - 2),)

    def send_lat(step, planes, side):
        src, dst, to = ((1, n_j + 1, lat_down), (n_j, 0, lat_up))[side]
        recv = lat_recv.at[step % 2, len(planes) - 1]
        for k in planes:
            remote(
                field.at[step, k, src, inner, :], field.at[step, k, dst, inner, :],
                lat_send, recv, {"lat": to},
            ).start()

    def send_lon(step, planes):
        recv = lon_recv.at[step % 2, len(planes) - 1]
        for src, dst, to in ((PAD, PAD + n_i, lon_down), (PAD + n_i - 1, PAD - 1, lon_up)):
            for k in planes:
                remote(
                    field.at[step, k, whole_j, pl.ds(src, 1), :],
                    field.at[step, k, whole_j, pl.ds(dst, 1), :],
                    lon_send, recv, {"lon": to},
                ).start()

    def wait_sides(step, planes):
        count = 2 if len(planes) == 2 else n_k - 2
        k = pl.ds(1, count)
        wait_for(field.at[step, k, pl.ds(0, 2), inner, :], lat_recv.at[step % 2, len(planes) - 1])
        wait_for(
            field.at[step, k, whole_j, pl.ds(PAD, 2), :], lon_recv.at[step % 2, len(planes) - 1]
        )

    def stat_copies(j):
        return [
            remote(
                own.at[j - 1], others.at[n_lev - 1 - away, j - 1],
                stat_send, stat_recv.at[n_lev - 1 - away, j - 1],
                {"lev": lax.rem(lev + away, n_lev)},
            )
            for away in range(1, n_lev)
        ]

    def update(step, k, j):
        for low in range(0, n_i, chunk):
            r = PAD + low
            middle = field[step, k, j, pl.ds(r, chunk), :]
            spread = (
                field[step, k, j - 1, pl.ds(r, chunk), :] + field[step, k, j + 1, pl.ds(r, chunk), :]
                + field[step, k, j, pl.ds(r - 1, chunk), :] + field[step, k, j, pl.ds(r + 1, chunk), :]
                + field[step, k - 1, j, pl.ds(r, chunk), :] + field[step, k + 1, j, pl.ds(r, chunk), :]
                - 6.0 * middle
            )
            rows = pl.ds(low, chunk)
            value = middle + coeff[k - 1, j - 1, rows, :] * spread + forcing[k - 1, j - 1, rows, :]
            if step == STEPS - 1:
                last[k - 1, j - 1, rows, :] = value
                place = pl.ds(low * n_k + k - 1, chunk, stride=n_k)
                tracer_end[j - 1, place, :] = value
            else:
                field[step + 1, k, j, pl.ds(r, chunk), :] = value

    def summarise(j):
        for low in range(0, n_i, chunk):
            rows = pl.ds(low, chunk)
            total = last[0, j - 1, rows, :]
            for k in range(1, n_k):
                total = total + last[k, j - 1, rows, :]
            mean = total * (1.0 / n_k)
            squares = jnp.zeros_like(mean)
            for k in range(n_k):
                moved = last[k, j - 1, rows, :] - mean
                squares = squares + moved * moved
            own[j - 1, 0, rows, :] = mean
            own[j - 1, 1, rows, :] = squares

    def over_k(first, end, body):
        def wrapped(k, carry):
            body(k)
            return carry
        lax.fori_loop(first, end, wrapped, 0)

    for j in range(1, n_j + 1):
        for piece in pieces(j):
            for k in (0, n_k - 1):
                load_edge(j, k, piece).start()

    barrier = pltpu.get_barrier_semaphore()

    def greet(axis, place, extent, sem):
        for away in others_near(extent):
            pl.semaphore_signal(
                sem, inc=1, device_id={axis: lax.rem(place + away, extent)}, device_id_type=MESH
            )

    sides = (("lat", lat, n_lat), ("lon", lon, n_lon))
    pairs = [extent % 2 == 0 for _, _, extent in sides]
    expected = n_lev - 1
    for away in range(1, n_lev):
        pl.semaphore_signal(
            barrier, inc=1, device_id={"lev": lax.rem(lev + away, n_lev)}, device_id_type=MESH
        )
    for paired, (axis, place, extent) in zip(pairs, sides):
        if paired:
            pl.when(lax.rem(place, 2) == 0)(functools.partial(greet, axis, place, extent, barrier))
            expected = expected + lax.rem(place, 2) * len(others_near(extent))
        else:
            greet(axis, place, extent, barrier)
            expected = expected + len(others_near(extent))
    with jax.named_scope("barrier"):
        pl.semaphore_wait(barrier, expected)
    for j in range(1, n_j + 1):
        for piece in pieces(j):
            low, size = piece
            sem = 3 + n_j if (j == 1 and low > 0) else 2 + j
            wait_for(field.at[0, pl.ds(1, 2), j, pl.ds(PAD + low, size), :], load_sem.at[sem])
            send_lev(0, j, piece)
    over_k(1, n_k - 1, lambda k: load(0, k, 0).start())
    for which in (1, 2):
        over_k(0, n_k, lambda k: load(which, k, which).start())
    for n, (paired, (axis, place, extent)) in enumerate(zip(pairs, sides)):
        if paired:
            @pl.when(lax.rem(place, 2) == 1)
            def _():
                greet(axis, place, extent, ready.at[n])

            @pl.when(lax.rem(place, 2) == 0)
            def _():
                pl.semaphore_wait(ready.at[n], len(others_near(extent)))

    for side in (0, 1):
        send_lat(0, edges, side)
    send_lon(0, edges)
    with jax.named_scope("load"):
        wait_for(field.at[0, pl.ds(1, n_k - 2), whole_j, inner, :], load_sem.at[0])
    for side in (0, 1):
        send_lat(0, middle, side)
    send_lon(0, middle)
    with jax.named_scope("load_rest"):
        wait_for(coeff, load_sem.at[1])
        wait_for(forcing, load_sem.at[2])

    def inside(step):
        with jax.named_scope(f"sides{step}"):
            wait_sides(step, middle)

        def body(k):
            def across(j, carry):
                update(step, k, j)
                return carry
            lax.fori_loop(1, n_j + 1, across, 0)

        with jax.named_scope(f"inside{step}"):
            over_k(2, n_k, body)
        if step < STEPS - 1:
            for side in (0, 1):
                send_lat(step + 1, middle, side)
            send_lon(step + 1, middle)

    def outside(step):
        with jax.named_scope(f"face_sides{step}"):
            wait_sides(step, edges)
        for j in range(1, n_j + 1):
            with jax.named_scope(f"lev{step}_{j}"):
                wait_lev(step, j)
            with jax.named_scope(f"face{step}_{j}"):
                update(step, 1, j)
                update(step, n_k, j)
            if step < STEPS - 1:
                send_lev(step + 1, j)
                for side, edge in ((0, 1), (1, n_j)):
                    if j == edge:
                        send_lat(step + 1, edges, side)
            else:
                with jax.named_scope(f"sum{j}"):
                    summarise(j)
                @pl.when(first_half)
                def _():
                    for copy in stat_copies(j):
                        copy.start()
        if step < STEPS - 1:
            send_lon(step + 1, edges)

    for step in range(STEPS):
        inside(step)
        outside(step)

    @pl.when(first_half)
    def _():
        for j in range(1, n_j + 1):
            with jax.named_scope(f"stat{j}"):
                for copy in stat_copies(j):
                    copy.wait_recv()
        wait_for(others, stat_send)

    with jax.named_scope("sent"):
        wait_for(field.at[:, pl.ds(0, 2), whole_j, inner, :], lev_send)
        wait_for(field.at[:, pl.ds(1, n_k), pl.ds(0, 2), inner, :], lat_send)
        wait_for(field.at[:, pl.ds(1, n_k), whole_j, pl.ds(PAD, 2), :], lon_send)


def combine(shape, n_lev, j, last, own, others, place_of):
    n_j, n_i, n_k, _ = shape
    chunk = rows_of(n_i)
    for low in range(0, n_i, chunk):
        rows = pl.ds(low, chunk)
        means = [own[j, 0, rows, :]] + [others[p, j, 0, rows, :] for p in range(n_lev - 1)]
        mean = functools.reduce(jnp.add, means) * (1.0 / n_lev)
        squares = own[j, 1, rows, :]
        for p in range(n_lev - 1):
            squares = squares + others[p, j, 1, rows, :]
        for part in means:
            squares = squares + n_k * ((part - mean) * (part - mean))
        scale = lax.rsqrt(squares * (1.0 / (n_k * n_lev)) + EPSILON)
        for k in range(n_k):
            place = pl.ds(low * n_k + k, chunk, stride=n_k)
            place_of[place, :] = (last[k, j, rows, :] - mean) * scale


def write_tracer(tracer_end, out, token, sem):
    copy = pltpu.make_async_copy(tracer_end, out, sem)
    copy.start()
    token[...] = jnp.zeros_like(token)
    copy.wait()


def second_kernel(
    sizes, shape, last, own, early, token, others, standardized, send_sem, recv_sem,
):
    n_j, n_i, _, _ = shape
    n_lev = sizes[2]
    lat, lev = lax.axis_index("lat"), lax.axis_index("lev")
    second_half = lax.rem(lat, 2) == 1

    def copies(j):
        return [
            pltpu.make_async_remote_copy(
                src_ref=own.at[j], dst_ref=others.at[n_lev - 1 - away, j],
                send_sem=send_sem, recv_sem=recv_sem.at[n_lev - 1 - away, j],
                device_id={"lev": lax.rem(lev + away, n_lev)}, device_id_type=MESH,
            )
            for away in range(1, n_lev)
        ]

    @pl.when(second_half)
    def _():
        barrier = pltpu.get_barrier_semaphore()
        for away in range(1, n_lev):
            pl.semaphore_signal(
                barrier, inc=1, device_id={"lev": lax.rem(lev + away, n_lev)}, device_id_type=MESH
            )
        with jax.named_scope("barrier2"):
            pl.semaphore_wait(barrier, n_lev - 1)
        for j in range(n_j):
            for copy in copies(j):
                copy.start()

    @pl.when(lax.rem(lat, 2) == 0)
    def _():
        others[...] = early[...]

    for j in range(n_j):
        @pl.when(second_half)
        def _():
            with jax.named_scope(f"late{j}"):
                for copy in copies(j):
                    copy.wait_recv()

        if j < n_j - 1:
            combine(shape, n_lev, j, last, own, others, standardized.at[j])

    @pl.when(second_half)
    def _():
        pltpu.make_async_copy(others, others, send_sem).wait()


def finish_kernel(shape, n_lev, last, own, others, ready, out, final, sem):
    n_j = shape[0]
    most = pl.ds(0, n_j - 1)
    earlier = pltpu.make_async_copy(ready.at[most], out.at[most], sem.at[0])
    latest = pltpu.make_async_copy(final, out.at[n_j - 1], sem.at[1])
    earlier.start()
    combine(shape, n_lev, n_j - 1, last, own, others, final)
    latest.start()
    earlier.wait()
    latest.wait()


def on_device(sizes, tracer, diffusivity, source):
    shape = tracer.shape
    n_j, n_i, n_k, levels = shape
    n_lev = sizes[2]
    f32 = jnp.float32
    sem = pltpu.SemaphoreType.DMA
    flat = (n_j, n_i * n_k, levels)
    parts = (
        pltpu.VMEM((n_k, n_j, n_i, levels), f32),
        pltpu.VMEM(flat, f32),
        pltpu.VMEM((n_j, 2, n_i, levels), f32),
        pltpu.VMEM((n_lev - 1, n_j, 2, n_i, levels), f32),
    )
    last, tracer_end, own, early = pl.pallas_call(
        functools.partial(steps_kernel, sizes, shape),
        out_shape=parts,
        in_specs=[pl.BlockSpec(memory_space=pl.ANY)] * 3,
        out_specs=(pl.BlockSpec(memory_space=pltpu.VMEM),) * len(parts),
        scratch_shapes=[
            pltpu.VMEM((STEPS, n_k + 2, n_j + 2, n_i + 2 * PAD, levels), f32),
            pltpu.VMEM((n_k, n_j, n_i, levels), f32),
            pltpu.VMEM((n_k, n_j, n_i, levels), f32),
            sem((n_j + 4,)),
            sem, sem((2, n_j)),
            sem, sem((2, 2)),
            sem, sem((2, 2)),
            sem, sem((n_lev - 1, n_j)),
            pltpu.SemaphoreType.REGULAR((2,)),
        ],
        compiler_params=pltpu.CompilerParams(
            collective_id=0, has_side_effects=True, vmem_limit_bytes=48 * 1024 * 1024,
        ),
    )(tracer, diffusivity, source)
    in_vmem, in_hbm = pl.BlockSpec(memory_space=pltpu.VMEM), pl.BlockSpec(memory_space=pl.ANY)
    tracer_end, token = pl.pallas_call(
        write_tracer,
        out_shape=(jax.ShapeDtypeStruct(flat, f32), pltpu.VMEM((8, levels), f32)),
        in_specs=[in_vmem],
        out_specs=(in_hbm, in_vmem),
        scratch_shapes=[sem],
        compiler_params=pltpu.CompilerParams(vmem_limit_bytes=1024 * 1024),
    )(tracer_end)
    others, standardized = pl.pallas_call(
        functools.partial(second_kernel, sizes, shape),
        out_shape=(parts[3], pltpu.VMEM(flat, f32)),
        in_specs=[in_vmem] * 4,
        out_specs=(in_vmem,) * 2,
        scratch_shapes=[sem, sem((n_lev - 1, n_j))],
        compiler_params=pltpu.CompilerParams(
            collective_id=1, has_side_effects=True, vmem_limit_bytes=8 * 1024 * 1024,
        ),
    )(last, own, early, token)
    standardized = pl.pallas_call(
        functools.partial(finish_kernel, shape, n_lev),
        out_shape=jax.ShapeDtypeStruct(flat, f32),
        in_specs=[in_vmem] * 4,
        out_specs=in_hbm,
        scratch_shapes=[pltpu.VMEM(flat[1:], f32), sem((2,))],
        compiler_params=pltpu.CompilerParams(vmem_limit_bytes=4 * 1024 * 1024),
    )(last, own, others, standardized)
    return standardized.reshape(shape), tracer_end.reshape(shape)


def solution(mesh):
    sizes = (mesh.shape["lat"], mesh.shape["lon"], mesh.shape["lev"])
    spec = P(("unit", "lat"), "lon", "lev", None)
    return jax.shard_map(
        functools.partial(on_device, sizes),
        mesh=mesh,
        in_specs=(spec, spec, spec),
        out_specs=(spec, spec),
        check_vma=False,
    )
```

```python
import functools

import jax
import jax.numpy as jnp
from jax import lax
from jax.experimental import pallas as pl
from jax.experimental.pallas import tpu as pltpu
from jax.sharding import PartitionSpec as P

STEPS = 4
PAD = 8
EPSILON = 0.0001
MESH = pl.DeviceIdType.MESH


def rows_of(extent):
    for rows in (32, 16, 8):
        if extent % rows == 0:
            return rows
    return extent


def others_near(extent):
    return sorted({1, extent - 1})


def steps_kernel(
    sizes, shape, tracer, diffusivity, source, last, tracer_end, own, others,
    field, coeff, forcing,
    load_sem, lev_send, lev_recv, lat_send, lat_recv, lon_send, lon_recv, stat_send, stat_recv, ready,
):
    n_j, n_i, n_k, _ = shape
    n_lat, n_lon, n_lev = sizes
    inner = pl.ds(PAD, n_i)
    whole_j = pl.ds(1, n_j)
    chunk = rows_of(n_i)
    lat, lon, lev = lax.axis_index("lat"), lax.axis_index("lon"), lax.axis_index("lev")
    lat_up, lat_down = lax.rem(lat + 1, n_lat), lax.rem(lat + n_lat - 1, n_lat)
    lon_up, lon_down = lax.rem(lon + 1, n_lon), lax.rem(lon + n_lon - 1, n_lon)
    lev_up, lev_down = lax.rem(lev + 1, n_lev), lax.rem(lev + n_lev - 1, n_lev)

    first_half = lax.rem(lat, 2) == 0

    def load(which, k, sem):
        array = (tracer, diffusivity, source)[which]
        if which == 0:
            target = field.at[0, k + 1, whole_j, inner, :]
        else:
            target = (coeff, forcing)[which - 1].at[k]
        return pltpu.make_async_copy(array.at[:, :, k, :], target, load_sem.at[sem])

    first = chunk if n_i > chunk else n_i

    def pieces(j):
        if j > 1 or first == n_i:
            return ((0, n_i),)
        return ((0, first), (first, n_i - first))

    def load_edge(j, k, piece):
        low, size = piece
        sem = 3 + n_j if (j == 1 and low > 0) else 2 + j
        return pltpu.make_async_copy(
            tracer.at[j - 1, pl.ds(low, size), k, :],
            field.at[0, k + 1, j, pl.ds(PAD + low, size), :], load_sem.at[sem],
        )

    def wait_for(ref, sem):
        pltpu.make_async_copy(ref, ref, sem).wait()

    def remote(src, dst, send, recv, device):
        return pltpu.make_async_remote_copy(
            src_ref=src, dst_ref=dst, send_sem=send, recv_sem=recv,
            device_id=device, device_id_type=MESH,
        )

    def send_lev(step, j, piece=None):
        low, size = piece or (0, n_i)
        rows = pl.ds(PAD + low, size)
        recv = lev_recv.at[step % 2, j - 1]
        for edge, halo, to in ((1, n_k + 1, lev_down), (n_k, 0, lev_up)):
            src = field.at[step, edge, j, rows, :]
            remote(src, field.at[step, halo, j, rows, :], lev_send, recv, {"lev": to}).start()

    def wait_lev(step, j):
        wait_for(field.at[step, pl.ds(0, 2), j, inner, :], lev_recv.at[step % 2, j - 1])

    edges, middle = (pl.ds(1, 1), pl.ds(n_k, 1)), (pl.ds(2, n_k - 2),)

    def send_lat(step, planes, side):
        src, dst, to = ((1, n_j + 1, lat_down), (n_j, 0, lat_up))[side]
        recv = lat_recv.at[step % 2, len(planes) - 1]
        for k in planes:
            remote(
                field.at[step, k, src, inner, :], field.at[step, k, dst, inner, :],
                lat_send, recv, {"lat": to},
            ).start()

    def send_lon(step, planes):
        recv = lon_recv.at[step % 2, len(planes) - 1]
        for src, dst, to in ((PAD, PAD + n_i, lon_down), (PAD + n_i - 1, PAD - 1, lon_up)):
            for k in planes:
                remote(
                    field.at[step, k, whole_j, pl.ds(src, 1), :],
                    field.at[step, k, whole_j, pl.ds(dst, 1), :],
                    lon_send, recv, {"lon": to},
                ).start()

    def wait_sides(step, planes):
        count = 2 if len(planes) == 2 else n_k - 2
        k = pl.ds(1, count)
        wait_for(field.at[step, k, pl.ds(0, 2), inner, :], lat_recv.at[step % 2, len(planes) - 1])
        wait_for(
            field.at[step, k, whole_j, pl.ds(PAD, 2), :], lon_recv.at[step % 2, len(planes) - 1]
        )

    def stat_copies(j):
        return [
            remote(
                own.at[j - 1], others.at[n_lev - 1 - away, j - 1],
                stat_send, stat_recv.at[n_lev - 1 - away, j - 1],
                {"lev": lax.rem(lev + away, n_lev)},
            )
            for away in range(1, n_lev)
        ]

    def update(step, k, j):
        for low in range(0, n_i, chunk):
            r = PAD + low
            middle = field[step, k, j, pl.ds(r, chunk), :]
            spread = (
                field[step, k, j - 1, pl.ds(r, chunk), :] + field[step, k, j + 1, pl.ds(r, chunk), :]
                + field[step, k, j, pl.ds(r - 1, chunk), :] + field[step, k, j, pl.ds(r + 1, chunk), :]
                + field[step, k - 1, j, pl.ds(r, chunk), :] + field[step, k + 1, j, pl.ds(r, chunk), :]
                - 6.0 * middle
            )
            rows = pl.ds(low, chunk)
            value = middle + coeff[k - 1, j - 1, rows, :] * spread + forcing[k - 1, j - 1, rows, :]
            if step == STEPS - 1:
                last[k - 1, j - 1, rows, :] = value
                place = pl.ds(low * n_k + k - 1, chunk, stride=n_k)
                tracer_end[j - 1, place, :] = value
            else:
                field[step + 1, k, j, pl.ds(r, chunk), :] = value

    def summarise(j):
        for low in range(0, n_i, chunk):
            rows = pl.ds(low, chunk)
            total = last[0, j - 1, rows, :]
            for k in range(1, n_k):
                total = total + last[k, j - 1, rows, :]
            mean = total * (1.0 / n_k)
            squares = jnp.zeros_like(mean)
            for k in range(n_k):
                moved = last[k, j - 1, rows, :] - mean
                squares = squares + moved * moved
            own[j - 1, 0, rows, :] = mean
            own[j - 1, 1, rows, :] = squares

    def over_k(first, end, body):
        def wrapped(k, carry):
            body(k)
            return carry
        lax.fori_loop(first, end, wrapped, 0)

    for j in range(1, n_j + 1):
        for piece in pieces(j):
            for k in (0, n_k - 1):
                load_edge(j, k, piece).start()

    barrier = pltpu.get_barrier_semaphore()

    def greet(axis, place, extent, sem):
        for away in others_near(extent):
            pl.semaphore_signal(
                sem, inc=1, device_id={axis: lax.rem(lax.axis_index(axis) + away, extent)},
                device_id_type=MESH,
            )

    sides = (("lat", lat + 1, n_lat), ("lon", lon, n_lon))
    pairs = [extent % 2 == 0 for _, _, extent in sides]
    expected = n_lev - 1
    for away in range(1, n_lev):
        pl.semaphore_signal(
            barrier, inc=1, device_id={"lev": lax.rem(lev + away, n_lev)}, device_id_type=MESH
        )
    for paired, (axis, place, extent) in zip(pairs, sides):
        if paired:
            pl.when(lax.rem(place, 2) == 0)(functools.partial(greet, axis, place, extent, barrier))
            expected = expected + lax.rem(place, 2) * len(others_near(extent))
        else:
            greet(axis, place, extent, barrier)
            expected = expected + len(others_near(extent))
    with jax.named_scope("barrier"):
        pl.semaphore_wait(barrier, expected)
    for j in range(1, n_j + 1):
        for piece in pieces(j):
            low, size = piece
            sem = 3 + n_j if (j == 1 and low > 0) else 2 + j
            wait_for(field.at[0, pl.ds(1, 2), j, pl.ds(PAD + low, size), :], load_sem.at[sem])
            send_lev(0, j, piece)
    over_k(1, n_k - 1, lambda k: load(0, k, 0).start())
    for which in (1, 2):
        over_k(0, n_k, lambda k: load(which, k, which).start())
    for n, (paired, (axis, place, extent)) in enumerate(zip(pairs, sides)):
        if paired:
            @pl.when(lax.rem(place, 2) == 1)
            def _():
                greet(axis, place, extent, ready.at[n])

            @pl.when(lax.rem(place, 2) == 0)
            def _():
                pl.semaphore_wait(ready.at[n], len(others_near(extent)))

    for side in (0, 1):
        send_lat(0, edges, side)
    send_lon(0, edges)
    with jax.named_scope("load"):
        wait_for(field.at[0, pl.ds(1, n_k - 2), whole_j, inner, :], load_sem.at[0])
    for side in (0, 1):
        send_lat(0, middle, side)
    send_lon(0, middle)
    with jax.named_scope("load_rest"):
        wait_for(coeff, load_sem.at[1])
        wait_for(forcing, load_sem.at[2])

    def inside(step):
        with jax.named_scope(f"sides{step}"):
            wait_sides(step, middle)

        def body(k):
            def across(j, carry):
                update(step, k, j)
                return carry
            lax.fori_loop(1, n_j + 1, across, 0)

        with jax.named_scope(f"inside{step}"):
            over_k(2, n_k, body)
        if step < STEPS - 1:
            for side in (0, 1):
                send_lat(step + 1, middle, side)
            send_lon(step + 1, middle)

    def outside(step):
        with jax.named_scope(f"face_sides{step}"):
            wait_sides(step, edges)
        for j in range(1, n_j + 1):
            with jax.named_scope(f"lev{step}_{j}"):
                wait_lev(step, j)
            with jax.named_scope(f"face{step}_{j}"):
                update(step, 1, j)
                update(step, n_k, j)
            if step < STEPS - 1:
                send_lev(step + 1, j)
                for side, edge in ((0, 1), (1, n_j)):
                    if j == edge:
                        send_lat(step + 1, edges, side)
            else:
                with jax.named_scope(f"sum{j}"):
                    summarise(j)
                @pl.when(first_half)
                def _():
                    for copy in stat_copies(j):
                        copy.start()
        if step < STEPS - 1:
            send_lon(step + 1, edges)

    for step in range(STEPS):
        inside(step)
        outside(step)

    @pl.when(first_half)
    def _():
        for j in range(1, n_j + 1):
            with jax.named_scope(f"stat{j}"):
                for copy in stat_copies(j):
                    copy.wait_recv()
        wait_for(others, stat_send)

    with jax.named_scope("sent"):
        wait_for(field.at[:, pl.ds(0, 2), whole_j, inner, :], lev_send)
        wait_for(field.at[:, pl.ds(1, n_k), pl.ds(0, 2), inner, :], lat_send)
        wait_for(field.at[:, pl.ds(1, n_k), whole_j, pl.ds(PAD, 2), :], lon_send)


def combine(shape, n_lev, j, last, own, others, place_of):
    n_j, n_i, n_k, _ = shape
    chunk = rows_of(n_i)
    for low in range(0, n_i, chunk):
        rows = pl.ds(low, chunk)
        means = [own[j, 0, rows, :]] + [others[p, j, 0, rows, :] for p in range(n_lev - 1)]
        mean = functools.reduce(jnp.add, means) * (1.0 / n_lev)
        squares = own[j, 1, rows, :]
        for p in range(n_lev - 1):
            squares = squares + others[p, j, 1, rows, :]
        for part in means:
            squares = squares + n_k * ((part - mean) * (part - mean))
        scale = lax.rsqrt(squares * (1.0 / (n_k * n_lev)) + EPSILON)
        for k in range(n_k):
            place = pl.ds(low * n_k + k, chunk, stride=n_k)
            place_of[place, :] = (last[k, j, rows, :] - mean) * scale


def write_tracer(tracer_end, out, token, sem):
    copy = pltpu.make_async_copy(tracer_end, out, sem)
    copy.start()
    token[...] = jnp.zeros_like(token)
    copy.wait()


def second_kernel(
    sizes, shape, last, own, early, token, others, standardized, send_sem, recv_sem,
):
    n_j, n_i, _, _ = shape
    n_lev = sizes[2]
    lat, lev = lax.axis_index("lat"), lax.axis_index("lev")
    second_half = lax.rem(lat, 2) == 1

    def copies(j):
        return [
            pltpu.make_async_remote_copy(
                src_ref=own.at[j], dst_ref=others.at[n_lev - 1 - away, j],
                send_sem=send_sem, recv_sem=recv_sem.at[n_lev - 1 - away, j],
                device_id={"lev": lax.rem(lev + away, n_lev)}, device_id_type=MESH,
            )
            for away in range(1, n_lev)
        ]

    @pl.when(second_half)
    def _():
        barrier = pltpu.get_barrier_semaphore()
        for away in range(1, n_lev):
            pl.semaphore_signal(
                barrier, inc=1, device_id={"lev": lax.rem(lev + away, n_lev)}, device_id_type=MESH
            )
        with jax.named_scope("barrier2"):
            pl.semaphore_wait(barrier, n_lev - 1)
        for j in range(n_j):
            for copy in copies(j):
                copy.start()

    @pl.when(lax.rem(lat, 2) == 0)
    def _():
        others[...] = early[...]

    for j in range(n_j):
        @pl.when(second_half)
        def _():
            with jax.named_scope(f"late{j}"):
                for copy in copies(j):
                    copy.wait_recv()

        if j < n_j - 1:
            combine(shape, n_lev, j, last, own, others, standardized.at[j])

    @pl.when(second_half)
    def _():
        pltpu.make_async_copy(others, others, send_sem).wait()


def finish_kernel(shape, n_lev, last, own, others, ready, out, final, sem):
    n_j = shape[0]
    most = pl.ds(0, n_j - 1)
    earlier = pltpu.make_async_copy(ready.at[most], out.at[most], sem.at[0])
    latest = pltpu.make_async_copy(final, out.at[n_j - 1], sem.at[1])
    earlier.start()
    combine(shape, n_lev, n_j - 1, last, own, others, final)
    latest.start()
    earlier.wait()
    latest.wait()


def on_device(sizes, tracer, diffusivity, source):
    shape = tracer.shape
    n_j, n_i, n_k, levels = shape
    n_lev = sizes[2]
    f32 = jnp.float32
    sem = pltpu.SemaphoreType.DMA
    flat = (n_j, n_i * n_k, levels)
    parts = (
        pltpu.VMEM((n_k, n_j, n_i, levels), f32),
        pltpu.VMEM(flat, f32),
        pltpu.VMEM((n_j, 2, n_i, levels), f32),
        pltpu.VMEM((n_lev - 1, n_j, 2, n_i, levels), f32),
    )
    last, tracer_end, own, early = pl.pallas_call(
        functools.partial(steps_kernel, sizes, shape),
        out_shape=parts,
        in_specs=[pl.BlockSpec(memory_space=pl.ANY)] * 3,
        out_specs=(pl.BlockSpec(memory_space=pltpu.VMEM),) * len(parts),
        scratch_shapes=[
            pltpu.VMEM((STEPS, n_k + 2, n_j + 2, n_i + 2 * PAD, levels), f32),
            pltpu.VMEM((n_k, n_j, n_i, levels), f32),
            pltpu.VMEM((n_k, n_j, n_i, levels), f32),
            sem((n_j + 4,)),
            sem, sem((2, n_j)),
            sem, sem((2, 2)),
            sem, sem((2, 2)),
            sem, sem((n_lev - 1, n_j)),
            pltpu.SemaphoreType.REGULAR((2,)),
        ],
        compiler_params=pltpu.CompilerParams(
            collective_id=0, has_side_effects=True, vmem_limit_bytes=48 * 1024 * 1024,
        ),
    )(tracer, diffusivity, source)
    in_vmem, in_hbm = pl.BlockSpec(memory_space=pltpu.VMEM), pl.BlockSpec(memory_space=pl.ANY)
    tracer_end, token = pl.pallas_call(
        write_tracer,
        out_shape=(jax.ShapeDtypeStruct(flat, f32), pltpu.VMEM((8, levels), f32)),
        in_specs=[in_vmem],
        out_specs=(in_hbm, in_vmem),
        scratch_shapes=[sem],
        compiler_params=pltpu.CompilerParams(vmem_limit_bytes=1024 * 1024),
    )(tracer_end)
    others, standardized = pl.pallas_call(
        functools.partial(second_kernel, sizes, shape),
        out_shape=(parts[3], pltpu.VMEM(flat, f32)),
        in_specs=[in_vmem] * 4,
        out_specs=(in_vmem,) * 2,
        scratch_shapes=[sem, sem((n_lev - 1, n_j))],
        compiler_params=pltpu.CompilerParams(
            collective_id=1, has_side_effects=True, vmem_limit_bytes=8 * 1024 * 1024,
        ),
    )(last, own, early, token)
    standardized = pl.pallas_call(
        functools.partial(finish_kernel, shape, n_lev),
        out_shape=jax.ShapeDtypeStruct(flat, f32),
        in_specs=[in_vmem] * 4,
        out_specs=in_hbm,
        scratch_shapes=[pltpu.VMEM(flat[1:], f32), sem((2,))],
        compiler_params=pltpu.CompilerParams(vmem_limit_bytes=4 * 1024 * 1024),
    )(last, own, others, standardized)
    return standardized.reshape(shape), tracer_end.reshape(shape)


def solution(mesh):
    sizes = (mesh.shape["lat"], mesh.shape["lon"], mesh.shape["lev"])
    spec = P(("unit", "lat"), "lon", "lev", None)
    return jax.shard_map(
        functools.partial(on_device, sizes),
        mesh=mesh,
        in_specs=(spec, spec, spec),
        out_specs=(spec, spec),
        check_vma=False,
    )
```
